32 devices in a mesh: grp: 2 (over y), ep: 4 (over x, core), hid: 4 (over z).
Axes of the slice: x: 2, y: 2, z: 4, core: 2. Of those that a mesh axis runs over, the one named last changes fastest.
Arguments:
- tokens: bfloat16 [1024, 4096], P(('grp', 'ep')), parts along dimension 0, may hold values from -6 to 6
- expert_ids: int32 [1024, 2], P(('grp', 'ep')), parts along dimension 0, may hold values from 0 to 3, all different within a row; in each aligned block of 128 rows (0 to 127, 128 to 255, ...) at most 64 rows name the same one
- gate_probs: float32 [1024, 2], P(('grp', 'ep')), parts along dimension 0, may hold values from 0.05 to 1
- w_gate: bfloat16 [16, 4096, 384], P(('ep', 'hid')), may hold values from -0.09375 to 0.09375
- w_up: bfloat16 [16, 4096, 384], P(('ep', 'hid')), may hold values from -0.09375 to 0.09375
- w_down: bfloat16 [16, 384, 4096], P(('ep', 'hid')), may hold values from -0.15625 to 0.15625
Outputs:
- mixed_out: bfloat16 [1024, 4096], P(('grp', 'ep'), 'hid'), parts along dimension 0
The draws below stay inside these ranges and needn't reach their ends.
There are 2 independent parts, one for each index of `grp`. The reference program is written for one: setup_inputs(seed, part) draws one part's arguments, and reference() takes and returns one part's arrays. A program takes and returns all parts, laid end to end along the dimension named above; an argument that names none is the same for every part. Nothing has to cross between parts.
Inputs may be any that keep to these rules, and one draw needn't show every extreme that they name: `expert_ids`: each token names 2 different experts. Among the 128 tokens of one index of ep (aligned blocks of rows) no expert is named by more than 64 tokens, and in every draw some expert is named by exactly 64 tokens of some block.
All inputs are finite; a program needn't handle non-finite values.
Results may differ from the reference program's by a relative error of at most 0.0085.
Values may be sent and summed in bfloat16 or wider, within the bound.
A program may use at most 128 MiB of HBM per device.

```python
import math
import jax
import jax.numpy as jnp
import numpy as np
from jax import lax

D = 4096
HIDDEN_SIZE = 1536
QUARTERS = 4
TOK_EP = 128
EXPERTS = 4
TOP = 2
CAP = 64
TOKENS = 512
N_EP = 4


def levels(own_key, dims, split, smallest, largest):
    def one(dim, blocks):
        steps = jax.random.uniform(jax.random.fold_in(jax.random.fold_in(own_key, 6), dim), (blocks,), jnp.float32, smallest / len(split), largest / len(split))
        return jnp.repeat(jnp.exp(steps), dims[dim] // blocks).reshape((-1,) + (1,) * (len(dims) - dim - 1))

    loudness = one(*split[0])
    for cut in split[1:]:
        loudness = loudness * one(*cut)
    return loudness


def shared_out(own_key, own, number, rows, count, top, most, lean):
    order = jax.random.permutation(own_key, count)
    crowded, common = shares(count, rows * top, most, lean, True), shares(count, rows * top, most, lean, False)
    places = jnp.arange(count)

    def named(tallies, turn):
        used = int((tallies > 0).sum())
        fixed = max(1, used // 4)
        passed = fixed + (places - fixed + turn * (used - fixed)) % max(1, count - fixed)
        return jnp.zeros((count,), jnp.int32).at[order[jnp.where(places < fixed, places, passed)]].set(jnp.asarray(tallies, jnp.int32))

    tallies = jnp.where(number % 4 == 0, named(crowded, number // 4), named(common, number - number // 4 - 1))
    mixed = jax.random.permutation(jax.random.fold_in(own, 3), count)
    donor, sink = mixed[0:count // 2 * 2:2], mixed[1:count // 2 * 2:2]
    room = jnp.minimum(tallies[donor] - 1, most - tallies[sink]) // 2
    room = jnp.where((donor == order[0]) | (sink == order[0]) | (tallies[sink] == 0), 0, jnp.maximum(room, 0))
    passed = jax.random.randint(jax.random.fold_in(own, 4), (count // 2,), 0, 1 << 20) % (room + 1)
    tallies = tallies.at[donor].add(-passed).at[sink].add(passed)
    items = jnp.searchsorted(jnp.cumsum(tallies), jnp.arange(rows * top), side="right").astype(jnp.int32)
    listing = items.reshape(top, rows).T
    listing = listing[jax.random.permutation(jax.random.fold_in(own, 1), rows)]
    turn = jax.random.randint(jax.random.fold_in(own, 2), (rows, 1), 0, top)
    return jnp.take_along_axis(listing, (jnp.arange(top)[None, :] + turn) % top, axis=1)


def shares(count, total, reach, slope, full):
    loads = [(1 << 20) // math.isqrt(standing ** slope) + 1 for standing in range(1, count + 1)]
    largest = reach if full else min(reach, max(-(-total // count), total * loads[0] // sum(loads)))
    least = 1 if total - largest >= count - 1 else 0
    given, rest = [largest] + [least] * (count - 1), total - largest - least * (count - 1)
    while rest > 0:
        movable = [i for i in range(1, count) if given[i] < largest] or [i for i in range(1, count) if given[i] < reach]
        pool, left = sum([loads[i] for i in movable]), rest
        for i in movable:
            extra = min(reach - given[i], max(1, left * loads[i] // pool), rest)
            given[i] = given[i] + extra
            rest = rest - extra
    return np.array(given)


def noise(own_key, extent, width, most, cuts=(), kind=jnp.bfloat16):
    array = width * jax.random.normal(own_key, extent, jnp.float32)
    if cuts:
        array = array * levels(own_key, extent, cuts, -0.22, 0.18)
    return jnp.clip(array, -most, most).astype(kind)


def setup_inputs(seed: int = 0, part: int = 0) -> dict:
    keys = jax.random.split(jax.random.key(seed), 7)
    part_keys = jax.random.split(jax.random.fold_in(keys[6], part), 7)
    tokens = noise(part_keys[0], (TOKENS, D), 1.0, 6.0, ((0, 4),))
    expert_ids_keys = jax.random.split(jax.random.fold_in(part_keys[1], 1), TOKENS // TOK_EP)
    expert_ids_turns = jax.random.permutation(jax.random.fold_in(part_keys[1], 3), TOKENS // TOK_EP)
    expert_ids = jax.vmap(lambda own, number: shared_out(jax.random.fold_in(part_keys[1], 2), own, number, TOK_EP, EXPERTS, TOP, CAP, 2))(expert_ids_keys, expert_ids_turns).reshape((TOKENS, TOP))
    gate_probs = jnp.clip(jnp.exp(math.log(1.0) - 2.9957323 * jax.random.uniform(part_keys[2], (TOKENS, TOP), jnp.float32) ** levels(part_keys[2], (TOKENS, TOP), ((0, 4),), -0.2, 0.2)), 0.05, 1.0)
    w_gate = noise(keys[3], (EXPERTS * QUARTERS, D, HIDDEN_SIZE // QUARTERS), D ** -0.5, 0.09375, ((0, 16),))
    w_up = noise(keys[4], (EXPERTS * QUARTERS, D, HIDDEN_SIZE // QUARTERS), D ** -0.5, 0.09375, ((0, 16),))
    w_down = noise(keys[5], (EXPERTS * QUARTERS, HIDDEN_SIZE // QUARTERS, D), HIDDEN_SIZE ** -0.5, 0.15625, ((0, 16),))
    return {"tokens": tokens, "expert_ids": expert_ids, "gate_probs": gate_probs, "w_gate": w_gate, "w_up": w_up, "w_down": w_down}


def reference(tokens, expert_ids, gate_probs, w_gate, w_up, w_down):
    tok_total, model_width = tokens.shape
    pick_count = expert_ids.shape[1]
    experts = w_gate.shape[0] // QUARTERS
    quarter_width = w_gate.shape[2]
    slots_each = N_EP * CAP
    grouped = expert_ids.reshape(N_EP, TOK_EP * pick_count)
    onehot = (grouped[:, :, None] == jnp.arange(experts, dtype=jnp.int32)[None, None, :]).astype(jnp.int32)
    before = jnp.cumsum(onehot, axis=1) - onehot
    position = jnp.sum(before * onehot, axis=2).astype(jnp.int32)
    block_index = jnp.arange(N_EP, dtype=jnp.int32)[:, None]
    slot_index = (grouped * slots_each + block_index * CAP + position).reshape(-1).astype(jnp.int32)
    routed_rows = jnp.repeat(tokens, pick_count, axis=0)
    buffer = jnp.zeros((experts * slots_each, model_width), tokens.dtype)
    buffer = buffer.at[slot_index].set(routed_rows).reshape(experts, slots_each, model_width)
    gate_stack = w_gate.reshape(experts, QUARTERS, model_width, quarter_width)
    up_stack = w_up.reshape(experts, QUARTERS, model_width, quarter_width)
    down_stack = w_down.reshape(experts, QUARTERS, quarter_width, model_width)

    def expert_fn(operands):
        expert_rows, gate_matrix, up_matrix, down_matrix = operands
        running = jnp.zeros((expert_rows.shape[0], model_width), jnp.float32)
        for index in range(QUARTERS):
            gate_act = jnp.dot(expert_rows, gate_matrix[index], preferred_element_type=jnp.float32)
            up_act = jnp.dot(expert_rows, up_matrix[index], preferred_element_type=jnp.float32)
            hidden = (jax.nn.silu(gate_act) * up_act).astype(jnp.bfloat16)
            piece_sum = jnp.dot(hidden, down_matrix[index], preferred_element_type=jnp.float32).astype(jnp.bfloat16)
            running = running + lax.optimization_barrier(piece_sum).astype(jnp.float32)
        return running

    outputs = lax.map(expert_fn, (buffer, gate_stack, up_stack, down_stack))
    picked = outputs.reshape(-1, model_width)[slot_index].reshape(tok_total, pick_count, model_width)
    weights = lax.optimization_barrier(gate_probs.astype(jnp.bfloat16)).astype(jnp.float32)
    mixed_out = jnp.einsum('tk,tkd->td', weights, picked, precision=lax.Precision.HIGHEST)
    return mixed_out.astype(jnp.bfloat16)
```

```python
import functools

import jax
import jax.numpy as jnp
from jax import lax
from jax.experimental import pallas as pl
from jax.experimental.pallas import tpu as pltpu
from jax.sharding import PartitionSpec as P

QUARTERS = 4
IN_CHUNKS = 4
HAND_OVER = 1
HELD_BACK = 2
RETURN_STEP = 256
MESH = pl.DeviceIdType.MESH
F32 = jnp.float32
BF16 = jnp.bfloat16


def aligned(index, size):
    return pl.ds(pl.multiple_of(index * size, size), size)


def kernel(ep_count, hid_count, tokens_hbm, ids_hbm, probs_hbm, w_gate, w_up, w_down, out,
           tokens, ids, probs, gate_buf, up_buf, down_buf, key_t, combine, outgoing, sibling_out, slots,
           gate_acc, up_acc, hidden, partial, returned, mate_out, mate_in, far_out, far_in,
           load_sem, sib_sem, disp_send, disp_recv, fwd_send, fwd_recv, ret_send, ret_sib, ret_recv,
           mate_send, mate_recv, far_send, far_recv):
    ep = lax.axis_index("ep")
    hid = lax.axis_index("hid")
    groups = hid_count // QUARTERS
    group = hid // QUARTERS
    rows, width = tokens.shape
    picks = ids.shape[0]
    cap = slots.shape[1]
    half = width // 2
    pairs = ep_count // 2
    pair = ep // 2
    core = ep % 2
    sibling = pair * 2 + 1 - core
    side = hid % 2
    mate = hid + 1 - 2 * side
    columns = hid_count // 2
    column = hid // 2
    feat = width // hid_count
    chunks, step = returned.shape[1], returned.shape[4]
    wide = half // IN_CHUNKS

    barrier = pltpu.get_barrier_semaphore()
    for off in range(1, ep_count):
        pl.semaphore_signal(barrier, 1, device_id={"ep": lax.rem(ep + off, ep_count)}, device_id_type=MESH)
    pl.semaphore_signal(barrier, 1, device_id={"hid": mate}, device_id_type=MESH)
    for off in range(1, columns):
        pl.semaphore_signal(barrier, 1, device_id={"hid": lax.rem(hid + 2 * off, hid_count)}, device_id_type=MESH)

    loads = [pltpu.make_async_copy(src, dst, load_sem.at[i])
             for i, (src, dst) in enumerate(((ids_hbm, ids), (probs_hbm, probs), (tokens_hbm, tokens),
                                             (w_gate.at[0], gate_buf), (w_up.at[0], up_buf), (w_down.at[0], down_buf)))]
    for load in loads[:3]:
        load.start()
    loads[0].wait()
    loads[1].wait()

    name = lax.broadcasted_iota(jnp.int32, (128, rows), 0) * groups + group
    count = jnp.zeros((128, rows), F32)
    weight = jnp.zeros((128, rows), F32)
    gate_round = probs[...].astype(BF16).astype(F32)
    for k in range(picks):
        hit = ids[k:k + 1, :] == name
        count = jnp.where(hit, 1.0, count)
        weight = jnp.where(hit, gate_round[k:k + 1, :], weight)
    earlier = (lax.broadcasted_iota(jnp.int32, (rows, rows), 0)
               < lax.broadcasted_iota(jnp.int32, (rows, rows), 1)).astype(F32).astype(BF16)
    before = jnp.dot(count.astype(BF16), earlier, preferred_element_type=F32)
    place = jnp.where(count > 0.5, before, -1000.0)
    key_t[...] = place.astype(jnp.int32)

    def pick_rows(first, blocks):
        row = lax.broadcasted_iota(jnp.int32, (cap, rows), 0)
        parts = [(key_t[pl.ds(first + b, 1), :] == row).astype(F32).astype(BF16) for b in range(blocks)]
        return jnp.concatenate(parts, axis=0) if blocks > 1 else parts[0]

    loads[2].wait()
    for load in loads[3:]:
        load.start()
    others = [lax.rem(pair + off, pairs) for off in range(1, pairs)]
    for i, other in enumerate(others):
        chosen = pick_rows(2 * other, 2)
        for k in range(IN_CHUNKS):
            rows_out = jnp.dot(chosen, tokens[:, aligned(side * IN_CHUNKS + k, wide)], preferred_element_type=F32)
            outgoing[i, :, :, k * wide:(k + 1) * wide] = rows_out.astype(BF16).reshape(2, cap, wide)
    dispatch = [pltpu.make_async_remote_copy(
        src_ref=outgoing.at[i, to, :, pl.ds(k * wide, wide)],
        dst_ref=slots.at[ep, :, aligned(side * IN_CHUNKS + k, wide)],
        send_sem=disp_send.at[to, i, k], recv_sem=disp_recv.at[ep, k],
        device_id={"ep": 2 * other + to}, device_id_type=MESH)
        for k in range(IN_CHUNKS) for i, other in enumerate(others) for to in range(2)]
    pl.semaphore_wait(barrier, ep_count - 1 + 1 + columns - 1)

    @pl.when(core == 0)
    def _():
        for copy in dispatch:
            copy.start()

    sends = list(dispatch)
    tile = min(half, 512)
    chosen = pick_rows(sibling, 1)
    for col in range(0, width, tile):
        sibling_out[:, col:col + tile] = jnp.dot(
            chosen, tokens[:, col:col + tile], preferred_element_type=F32).astype(BF16)
    to_sibling = pltpu.make_async_remote_copy(
        src_ref=sibling_out, dst_ref=slots.at[ep], send_sem=sib_sem.at[0], recv_sem=sib_sem.at[1],
        device_id={"ep": sibling}, device_id_type=MESH)
    to_sibling.start()
    sends.append(to_sibling)
    chosen = pick_rows(ep, 1)
    for col in range(0, width, tile):
        slots[ep, :, col:col + tile] = jnp.dot(
            chosen, tokens[:, col:col + tile], preferred_element_type=F32).astype(BF16)

    lanes = lax.broadcasted_iota(jnp.int32, (rows, cap), 1)
    key = place.T.astype(jnp.int32)
    weight = weight.T
    for b in range(ep_count):
        combine[:, b * cap:(b + 1) * cap] = jnp.where(
            key[:, b:b + 1] == lanes, weight[:, b:b + 1], 0.0).astype(BF16)

    def activation(gate_act, up_act):
        return (gate_act / (1.0 + jnp.exp(-gate_act)) * up_act).astype(BF16)

    def act_step(stage, i, k, first=False, last=False):
        block = slots[2 * others[i] + stage, :, aligned(k, wide)]
        gate_act = jnp.dot(block, gate_buf[aligned(k, wide), :], preferred_element_type=F32)
        up_act = jnp.dot(block, up_buf[aligned(k, wide), :], preferred_element_type=F32)
        if not first:
            gate_act = gate_act + gate_acc[stage, i]
            up_act = up_act + up_acc[stage, i]
        if last:
            hidden[stage, others[i]] = activation(gate_act, up_act)
        else:
            gate_acc[stage, i] = gate_act
            up_acc[stage, i] = up_act

    pltpu.make_async_remote_copy(
        src_ref=sibling_out, dst_ref=slots.at[sibling], send_sem=sib_sem.at[0], recv_sem=sib_sem.at[1],
        device_id={"ep": sibling}, device_id_type=MESH).wait_recv()
    loads[3].wait()
    loads[4].wait()
    block = slots[pl.ds(2 * pair, 2)].reshape(2 * cap, width)
    value = activation(jnp.dot(block, gate_buf[...], preferred_element_type=F32),
                       jnp.dot(block, up_buf[...], preferred_element_type=F32))
    for stage in range(2):
        hidden[stage, pair] = value[stage * cap:(stage + 1) * cap]

    def forward(stage, i, k):
        landed = slots.at[2 * others[i] + stage, :, aligned(side * IN_CHUNKS + k, wide)]
        return pltpu.make_async_remote_copy(
            src_ref=landed, dst_ref=landed,
            send_sem=fwd_send.at[i, k, stage], recv_sem=fwd_recv.at[i, k, stage],
            device_id={"hid": mate}, device_id_type=MESH)

    def direct(stage, i, k):
        source = 2 * others[i] + stage
        landed = slots.at[source, :, aligned(side * IN_CHUNKS + k, wide)]
        pltpu.make_async_remote_copy(
            src_ref=landed, dst_ref=landed,
            send_sem=disp_send.at[0, i, k], recv_sem=disp_recv.at[source, k],
            device_id={"ep": source}, device_id_type=MESH).wait_recv()
        copy = forward(stage, i, k)
        copy.start()
        sends.append(copy)
        act_step(stage, i, side * IN_CHUNKS + k, first=k == 0)

    def relayed(stage, i, k):
        forward(stage, i, k).wait_recv()
        act_step(stage, i, (1 - side) * IN_CHUNKS + k, last=k == IN_CHUNKS - 1)

    pieces = [(i, k) for i in range(pairs - 1) for k in range(IN_CHUNKS)]

    elsewhere = [lax.rem(column + off, columns) for off in range(1, columns)]
    targets = [2 * c + 1 - side for c in elsewhere] + [2 * c + side for c in elsewhere] + [mate, hid]

    def give_back(stage):
        for s, target in enumerate(targets):
            for c in range(chunks):
                value = jnp.dot(hidden[stage].reshape(pairs * cap, -1), down_buf[:, aligned(target * chunks + c, step)],
                                preferred_element_type=F32)
                partial[stage, s, c] = value.astype(BF16).reshape(pairs, cap, step)
                for i, other in enumerate(others):
                    copy = pltpu.make_async_remote_copy(
                        src_ref=partial.at[stage, s, c, other], dst_ref=returned.at[s, c, ep],
                        send_sem=ret_send.at[stage, s, c, i], recv_sem=ret_recv.at[s, c, ep],
                        device_id={"ep": 2 * other + stage}, device_id_type=MESH)
                    copy.start()
                    sends.append(copy)

        @pl.when(core == stage)
        def _():
            for s in range(hid_count):
                for c in range(chunks):
                    returned[s, c, ep] = partial[stage, s, c, pair]

        @pl.when(core != stage)
        def _():
            for s in range(hid_count):
                for c in range(chunks):
                    back_to_sibling(stage, s, c).start()

    def back_to_sibling(stage, s, c):
        return pltpu.make_async_remote_copy(
            src_ref=partial.at[stage, s, c, pair], dst_ref=returned.at[s, c, ep],
            send_sem=ret_sib.at[s, c], recv_sem=ret_recv.at[s, c, ep],
            device_id={"ep": sibling}, device_id_type=MESH)

    for n, piece in enumerate(pieces):
        direct(0, *piece)
        if n == HAND_OVER:
            @pl.when(core == 1)
            def _():
                for copy in dispatch:
                    copy.start()
    held = len(pieces) - HELD_BACK
    for n, piece in enumerate(pieces):
        relayed(0, *piece)
        if n < held:
            direct(1, *pieces[n])
    loads[5].wait()
    give_back(0)
    for piece in pieces[held:]:
        direct(1, *piece)
    for piece in pieces:
        relayed(1, *piece)
    give_back(1)

    def to_mate(slot, c):
        return pltpu.make_async_remote_copy(
            src_ref=mate_out.at[slot, c], dst_ref=mate_in.at[slot, c],
            send_sem=mate_send.at[slot, c], recv_sem=mate_recv.at[slot, c],
            device_id={"hid": mate}, device_id_type=MESH)

    def to_far(slot, c, target):
        return pltpu.make_async_remote_copy(
            src_ref=far_out.at[slot, c], dst_ref=far_in.at[slot, c],
            send_sem=far_send.at[slot, c], recv_sem=far_recv.at[slot, c],
            device_id={"hid": target}, device_id_type=MESH)

    for s, target in enumerate(targets):
        for c in range(chunks):
            for off in range(1, ep_count):
                source = lax.rem(ep + off, ep_count)
                pltpu.make_async_remote_copy(
                    src_ref=returned.at[s, c, source], dst_ref=returned.at[s, c, source],
                    send_sem=ret_sib.at[s, c], recv_sem=ret_recv.at[s, c, source],
                    device_id={"ep": source}, device_id_type=MESH).wait_recv()
            total = jnp.dot(combine[...], returned[s, c].reshape(ep_count * cap, step), preferred_element_type=F32)
            if s < columns - 1 or s == 2 * columns - 2:
                slot = s if s < columns - 1 else columns - 1
                mate_out[slot, c] = total.astype(BF16)
                copy = to_mate(slot, c)
            elif s < 2 * columns - 2:
                slot = s - (columns - 1)
                to_mate(slot, c).wait_recv()
                far_out[slot, c] = (total + mate_in[slot, c].astype(F32)).astype(BF16)
                copy = to_far(slot, c, target)
            else:
                to_mate(columns - 1, c).wait_recv()
                total = total + mate_in[columns - 1, c].astype(F32)
                for slot in range(columns - 1):
                    to_far(slot, c, target).wait_recv()
                    total = total + far_in[slot, c].astype(F32)
                out[:, c * step:(c + 1) * step] = total.astype(BF16)
                continue
            copy.start()
            sends.append(copy)
    for s in range(hid_count):
        for c in range(chunks):
            back_to_sibling(1 - core, s, c).wait_send()
    for copy in sends:
        copy.wait_send()


def local(ep_count, hid_count, tokens, expert_ids, gate_probs, w_gate, w_up, w_down):
    rows, width = tokens.shape
    inner = w_gate.shape[2]
    picks = expert_ids.shape[1]
    cap = rows // 2
    feat = width // hid_count
    step = min(RETURN_STEP, feat)
    chunks = feat // step
    pairs = ep_count // 2
    columns = hid_count // 2
    others = max(pairs - 1, 1)
    far = max(columns - 1, 1)
    hbm = pl.BlockSpec(memory_space=pl.ANY)
    dma = pltpu.SemaphoreType.DMA
    return pl.pallas_call(
        functools.partial(kernel, ep_count, hid_count),
        out_shape=pltpu.VMEM((rows, feat), BF16),
        in_specs=[hbm] * 6,
        out_specs=pl.BlockSpec(memory_space=pltpu.VMEM),
        scratch_shapes=[
            pltpu.VMEM((rows, width), BF16),
            pltpu.VMEM((picks, rows), jnp.int32),
            pltpu.VMEM((picks, rows), F32),
            pltpu.VMEM((width, inner), BF16),
            pltpu.VMEM((width, inner), BF16),
            pltpu.VMEM((inner, width), BF16),
            pltpu.VMEM((128, rows), jnp.int32),
            pltpu.VMEM((rows, ep_count * cap), BF16),
            pltpu.VMEM((others, 2, cap, width // 2), BF16),
            pltpu.VMEM((cap, width), BF16),
            pltpu.VMEM((ep_count, cap, width), BF16),
            pltpu.VMEM((2, others, cap, inner), F32),
            pltpu.VMEM((2, others, cap, inner), F32),
            pltpu.VMEM((2, pairs, cap, inner), BF16),
            pltpu.VMEM((2, hid_count, chunks, pairs, cap, step), BF16),
            pltpu.VMEM((hid_count, chunks, ep_count, cap, step), BF16),
            pltpu.VMEM((columns, chunks, rows, step), BF16),
            pltpu.VMEM((columns, chunks, rows, step), BF16),
            pltpu.VMEM((far, chunks, rows, step), BF16),
            pltpu.VMEM((far, chunks, rows, step), BF16),
            dma((6,)),
            dma((2,)),
            dma((2, others, IN_CHUNKS)),
            dma((ep_count, IN_CHUNKS)),
            dma((others, IN_CHUNKS, 2)),
            dma((others, IN_CHUNKS, 2)),
            dma((2, hid_count, chunks, others)),
            dma((hid_count, chunks)),
            dma((hid_count, chunks, ep_count)),
            dma((columns, chunks)),
            dma((columns, chunks)),
            dma((far, chunks)),
            dma((far, chunks)),
        ],
        compiler_params=pltpu.CompilerParams(
            collective_id=0, has_side_effects=True, vmem_limit_bytes=60 * 2**20),
    )(tokens, expert_ids.T, gate_probs.T, w_gate, w_up, w_down)


def solution(mesh):
    in_specs = (
        P(("grp", "ep"), None),
        P(("grp", "ep"), None),
        P(("grp", "ep"), None),
        P(("ep", "hid"), None, None),
        P(("ep", "hid"), None, None),
        P(("ep", "hid"), None, None),
    )
    out_specs = P(("grp", "ep"), "hid")
    body = functools.partial(local, mesh.shape["ep"], mesh.shape["hid"])
    return jax.shard_map(body, mesh=mesh, in_specs=in_specs, out_specs=out_specs, check_vma=False)
```

```python
import functools

import jax
import jax.numpy as jnp
from jax import lax
from jax.experimental import pallas as pl
from jax.experimental.pallas import tpu as pltpu
from jax.sharding import PartitionSpec as P

QUARTERS = 4
IN_CHUNKS = 4
HAND_OVER = 1
HELD_BACK = 2
EARLY = (8, 4)
RETURN_STEP = 256
MESH = pl.DeviceIdType.MESH
F32 = jnp.float32
BF16 = jnp.bfloat16


def aligned(index, size):
    return pl.ds(pl.multiple_of(index * size, size), size)


def kernel(ep_count, hid_count, tokens_hbm, ids_hbm, probs_hbm, w_gate, w_up, w_down, out,
           tokens, ids, probs, gate_buf, up_buf, down_buf, key_t, combine, outgoing, sibling_out, slots,
           gate_acc, up_acc, hidden, partial, returned, mate_out, mate_in, far_out, far_in,
           load_sem, sib_sem, disp_send, disp_recv, fwd_send, fwd_recv, ret_send, ret_sib, ret_recv,
           mate_send, mate_recv, far_send, far_recv):
    ep = lax.axis_index("ep")
    hid = lax.axis_index("hid")
    groups = hid_count // QUARTERS
    group = hid // QUARTERS
    rows, width = tokens.shape
    picks = ids.shape[0]
    cap = slots.shape[1]
    half = width // 2
    pairs = ep_count // 2
    pair = ep // 2
    core = ep % 2
    sibling = pair * 2 + 1 - core
    side = hid % 2
    mate = hid + 1 - 2 * side
    columns = hid_count // 2
    column = hid // 2
    feat = width // hid_count
    chunks, step = returned.shape[1], returned.shape[4]
    wide = half // IN_CHUNKS

    barrier = pltpu.get_barrier_semaphore()
    for off in range(1, ep_count):
        pl.semaphore_signal(barrier, 1, device_id={"ep": lax.rem(ep + off, ep_count)}, device_id_type=MESH)
    pl.semaphore_signal(barrier, 1, device_id={"hid": mate}, device_id_type=MESH)
    for off in range(1, columns):
        pl.semaphore_signal(barrier, 1, device_id={"hid": lax.rem(hid + 2 * off, hid_count)}, device_id_type=MESH)

    loads = [pltpu.make_async_copy(src, dst, load_sem.at[i])
             for i, (src, dst) in enumerate(((ids_hbm, ids), (probs_hbm, probs), (tokens_hbm, tokens),
                                             (w_gate.at[0], gate_buf), (w_up.at[0], up_buf), (w_down.at[0], down_buf)))]
    for load in loads[:3]:
        load.start()
    loads[0].wait()
    loads[1].wait()

    name = lax.broadcasted_iota(jnp.int32, (128, rows), 0) * groups + group
    count = jnp.zeros((128, rows), F32)
    weight = jnp.zeros((128, rows), F32)
    gate_round = probs[...].astype(BF16).astype(F32)
    for k in range(picks):
        hit = ids[k:k + 1, :] == name
        count = jnp.where(hit, 1.0, count)
        weight = jnp.where(hit, gate_round[k:k + 1, :], weight)
    earlier = (lax.broadcasted_iota(jnp.int32, (rows, rows), 0)
               < lax.broadcasted_iota(jnp.int32, (rows, rows), 1)).astype(F32).astype(BF16)
    before = jnp.dot(count.astype(BF16), earlier, preferred_element_type=F32)
    place = jnp.where(count > 0.5, before, -1000.0)
    key_t[...] = place.astype(jnp.int32)

    def pick_rows(first, blocks):
        row = lax.broadcasted_iota(jnp.int32, (cap, rows), 0)
        parts = [(key_t[pl.ds(first + b, 1), :] == row).astype(F32).astype(BF16) for b in range(blocks)]
        return jnp.concatenate(parts, axis=0) if blocks > 1 else parts[0]

    loads[2].wait()
    for load in loads[3:]:
        load.start()
    others = [lax.rem(pair + off, pairs) for off in range(1, pairs)]
    for i, other in enumerate(others):
        chosen = pick_rows(2 * other, 2)
        for k in range(IN_CHUNKS):
            rows_out = jnp.dot(chosen, tokens[:, aligned(side * IN_CHUNKS + k, wide)], preferred_element_type=F32)
            outgoing[i, :, :, k * wide:(k + 1) * wide] = rows_out.astype(BF16).reshape(2, cap, wide)
    dispatch = [pltpu.make_async_remote_copy(
        src_ref=outgoing.at[i, to, :, pl.ds(k * wide, wide)],
        dst_ref=slots.at[ep, :, aligned(side * IN_CHUNKS + k, wide)],
        send_sem=disp_send.at[to, i, k], recv_sem=disp_recv.at[ep, k],
        device_id={"ep": 2 * other + to}, device_id_type=MESH)
        for k in range(IN_CHUNKS) for i, other in enumerate(others) for to in range(2)]
    pl.semaphore_wait(barrier, ep_count - 1 + 1 + columns - 1)

    @pl.when(core == 0)
    def _():
        for copy in dispatch:
            copy.start()

    sends = list(dispatch)
    tile = min(half, 512)
    chosen = pick_rows(sibling, 1)
    for col in range(0, width, tile):
        sibling_out[:, col:col + tile] = jnp.dot(
            chosen, tokens[:, col:col + tile], preferred_element_type=F32).astype(BF16)
    to_sibling = pltpu.make_async_remote_copy(
        src_ref=sibling_out, dst_ref=slots.at[ep], send_sem=sib_sem.at[0], recv_sem=sib_sem.at[1],
        device_id={"ep": sibling}, device_id_type=MESH)
    to_sibling.start()
    sends.append(to_sibling)
    chosen = pick_rows(ep, 1)
    for col in range(0, width, tile):
        slots[ep, :, col:col + tile] = jnp.dot(
            chosen, tokens[:, col:col + tile], preferred_element_type=F32).astype(BF16)

    lanes = lax.broadcasted_iota(jnp.int32, (rows, cap), 1)
    key = place.T.astype(jnp.int32)
    weight = weight.T
    for b in range(ep_count):
        combine[:, b * cap:(b + 1) * cap] = jnp.where(
            key[:, b:b + 1] == lanes, weight[:, b:b + 1], 0.0).astype(BF16)

    def activation(gate_act, up_act):
        return (gate_act / (1.0 + jnp.exp(-gate_act)) * up_act).astype(BF16)

    def act_step(stage, i, k, first=False, last=False):
        block = slots[2 * others[i] + stage, :, aligned(k, wide)]
        gate_act = jnp.dot(block, gate_buf[aligned(k, wide), :], preferred_element_type=F32)
        up_act = jnp.dot(block, up_buf[aligned(k, wide), :], preferred_element_type=F32)
        if not first:
            gate_act = gate_act + gate_acc[stage, i]
            up_act = up_act + up_acc[stage, i]
        if last:
            hidden[stage, others[i]] = activation(gate_act, up_act)
        else:
            gate_acc[stage, i] = gate_act
            up_acc[stage, i] = up_act

    pltpu.make_async_remote_copy(
        src_ref=sibling_out, dst_ref=slots.at[sibling], send_sem=sib_sem.at[0], recv_sem=sib_sem.at[1],
        device_id={"ep": sibling}, device_id_type=MESH).wait_recv()
    loads[3].wait()
    loads[4].wait()
    block = slots[pl.ds(2 * pair, 2)].reshape(2 * cap, width)
    value = activation(jnp.dot(block, gate_buf[...], preferred_element_type=F32),
                       jnp.dot(block, up_buf[...], preferred_element_type=F32))
    for stage in range(2):
        hidden[stage, pair] = value[stage * cap:(stage + 1) * cap]

    def forward(stage, i, k):
        landed = slots.at[2 * others[i] + stage, :, aligned(side * IN_CHUNKS + k, wide)]
        return pltpu.make_async_remote_copy(
            src_ref=landed, dst_ref=landed,
            send_sem=fwd_send.at[i, k, stage], recv_sem=fwd_recv.at[i, k, stage],
            device_id={"hid": mate}, device_id_type=MESH)

    def direct(stage, i, k):
        source = 2 * others[i] + stage
        landed = slots.at[source, :, aligned(side * IN_CHUNKS + k, wide)]
        pltpu.make_async_remote_copy(
            src_ref=landed, dst_ref=landed,
            send_sem=disp_send.at[0, i, k], recv_sem=disp_recv.at[source, k],
            device_id={"ep": source}, device_id_type=MESH).wait_recv()
        copy = forward(stage, i, k)
        copy.start()
        sends.append(copy)
        act_step(stage, i, side * IN_CHUNKS + k, first=k == 0)

    def relayed(stage, i, k):
        forward(stage, i, k).wait_recv()
        act_step(stage, i, (1 - side) * IN_CHUNKS + k, last=k == IN_CHUNKS - 1)

    pieces = [(i, k) for i in range(pairs - 1) for k in range(IN_CHUNKS)]

    elsewhere = [lax.rem(column + off, columns) for off in range(1, columns)]
    targets = [2 * c + 1 - side for c in elsewhere] + [2 * c + side for c in elsewhere] + [mate, hid]

    away = [(s, c) for s in range(columns - 1) for c in range(chunks)]
    for c in range(chunks):
        away += [(s, c) for s in range(columns - 1, 2 * columns - 1)]
    own = [(hid_count - 1, c) for c in range(chunks)]

    def give_back(stage, order):
        for s, c in order:
            target = targets[s]
            value = jnp.dot(hidden[stage].reshape(pairs * cap, -1), down_buf[:, aligned(target * chunks + c, step)],
                            preferred_element_type=F32)
            partial[stage, s, c] = value.astype(BF16).reshape(pairs, cap, step)
            for i, other in enumerate(others):
                copy = pltpu.make_async_remote_copy(
                    src_ref=partial.at[stage, s, c, other], dst_ref=returned.at[s, c, ep],
                    send_sem=ret_send.at[stage, s, c, i], recv_sem=ret_recv.at[s, c, ep],
                    device_id={"ep": 2 * other + stage}, device_id_type=MESH)
                copy.start()
                sends.append(copy)

        @pl.when(core == stage)
        def _():
            for s, c in order:
                returned[s, c, ep] = partial[stage, s, c, pair]

        @pl.when(core != stage)
        def _():
            for s, c in order:
                back_to_sibling(stage, s, c).start()

    def back_to_sibling(stage, s, c):
        return pltpu.make_async_remote_copy(
            src_ref=partial.at[stage, s, c, pair], dst_ref=returned.at[s, c, ep],
            send_sem=ret_sib.at[s, c], recv_sem=ret_recv.at[s, c, ep],
            device_id={"ep": sibling}, device_id_type=MESH)

    def to_mate(slot, c):
        return pltpu.make_async_remote_copy(
            src_ref=mate_out.at[slot, c], dst_ref=mate_in.at[slot, c],
            send_sem=mate_send.at[slot, c], recv_sem=mate_recv.at[slot, c],
            device_id={"hid": mate}, device_id_type=MESH)

    def to_far(slot, c, target):
        return pltpu.make_async_remote_copy(
            src_ref=far_out.at[slot, c], dst_ref=far_in.at[slot, c],
            send_sem=far_send.at[slot, c], recv_sem=far_recv.at[slot, c],
            device_id={"hid": target}, device_id_type=MESH)

    def gather(s, c):
        for off in range(1, ep_count):
            source = lax.rem(ep + off, ep_count)
            pltpu.make_async_remote_copy(
                src_ref=returned.at[s, c, source], dst_ref=returned.at[s, c, source],
                send_sem=ret_sib.at[s, c], recv_sem=ret_recv.at[s, c, source],
                device_id={"ep": source}, device_id_type=MESH).wait_recv()
        total = jnp.dot(combine[...], returned[s, c].reshape(ep_count * cap, step), preferred_element_type=F32)
        if s < columns - 1 or s == 2 * columns - 2:
            slot = s if s < columns - 1 else columns - 1
            mate_out[slot, c] = total.astype(BF16)
            copy = to_mate(slot, c)
        elif s < 2 * columns - 2:
            slot = s - (columns - 1)
            to_mate(slot, c).wait_recv()
            far_out[slot, c] = (total + mate_in[slot, c].astype(F32)).astype(BF16)
            copy = to_far(slot, c, targets[s])
        else:
            to_mate(columns - 1, c).wait_recv()
            total = total + mate_in[columns - 1, c].astype(F32)
            for slot in range(columns - 1):
                to_far(slot, c, targets[s]).wait_recv()
                total = total + far_in[slot, c].astype(F32)
            out[:, c * step:(c + 1) * step] = total.astype(BF16)
            return
        copy.start()
    def gather_on(which, order):
        @pl.when(core == which)
        def _():
            for s, c in order:
                gather(s, c)

    for n, piece in enumerate(pieces):
        direct(0, *piece)
        if n == HAND_OVER:
            @pl.when(core == 1)
            def _():
                for copy in dispatch:
                    copy.start()
    held = len(pieces) - HELD_BACK
    for n, piece in enumerate(pieces):
        relayed(0, *piece)
        if n < held:
            direct(1, *pieces[n])
    loads[5].wait()
    give_back(0, away)
    for piece in pieces[held:]:
        direct(1, *piece)
    first = EARLY[0]
    gather_on(0, away[:first])
    for piece in pieces:
        relayed(1, *piece)
    early = first + EARLY[1]
    gather_on(0, away[first:early])
    give_back(1, away)
    give_back(0, own)
    give_back(1, own)
    gather_on(1, away[:early])
    for s, c in away[early:] + own:
        gather(s, c)

    for s in range(hid_count):
        for c in range(chunks):
            back_to_sibling(1 - core, s, c).wait_send()
    for c in range(chunks):
        for slot in range(columns):
            to_mate(slot, c).wait_send()
        for slot in range(columns - 1):
            to_far(slot, c, targets[columns - 1 + slot]).wait_send()
    for copy in sends:
        copy.wait_send()


def local(ep_count, hid_count, tokens, expert_ids, gate_probs, w_gate, w_up, w_down):
    rows, width = tokens.shape
    inner = w_gate.shape[2]
    picks = expert_ids.shape[1]
    cap = rows // 2
    feat = width // hid_count
    step = min(RETURN_STEP, feat)
    chunks = feat // step
    pairs = ep_count // 2
    columns = hid_count // 2
    others = max(pairs - 1, 1)
    far = max(columns - 1, 1)
    hbm = pl.BlockSpec(memory_space=pl.ANY)
    dma = pltpu.SemaphoreType.DMA
    return pl.pallas_call(
        functools.partial(kernel, ep_count, hid_count),
        out_shape=pltpu.VMEM((rows, feat), BF16),
        in_specs=[hbm] * 6,
        out_specs=pl.BlockSpec(memory_space=pltpu.VMEM),
        scratch_shapes=[
            pltpu.VMEM((rows, width), BF16),
            pltpu.VMEM((picks, rows), jnp.int32),
            pltpu.VMEM((picks, rows), F32),
            pltpu.VMEM((width, inner), BF16),
            pltpu.VMEM((width, inner), BF16),
            pltpu.VMEM((inner, width), BF16),
            pltpu.VMEM((128, rows), jnp.int32),
            pltpu.VMEM((rows, ep_count * cap), BF16),
            pltpu.VMEM((others, 2, cap, width // 2), BF16),
            pltpu.VMEM((cap, width), BF16),
            pltpu.VMEM((ep_count, cap, width), BF16),
            pltpu.VMEM((2, others, cap, inner), F32),
            pltpu.VMEM((2, others, cap, inner), F32),
            pltpu.VMEM((2, pairs, cap, inner), BF16),
            pltpu.VMEM((2, hid_count, chunks, pairs, cap, step), BF16),
            pltpu.VMEM((hid_count, chunks, ep_count, cap, step), BF16),
            pltpu.VMEM((columns, chunks, rows, step), BF16),
            pltpu.VMEM((columns, chunks, rows, step), BF16),
            pltpu.VMEM((far, chunks, rows, step), BF16),
            pltpu.VMEM((far, chunks, rows, step), BF16),
            dma((6,)),
            dma((2,)),
            dma((2, others, IN_CHUNKS)),
            dma((ep_count, IN_CHUNKS)),
            dma((others, IN_CHUNKS, 2)),
            dma((others, IN_CHUNKS, 2)),
            dma((2, hid_count, chunks, others)),
            dma((hid_count, chunks)),
            dma((hid_count, chunks, ep_count)),
            dma((columns, chunks)),
            dma((columns, chunks)),
            dma((far, chunks)),
            dma((far, chunks)),
        ],
        compiler_params=pltpu.CompilerParams(
            collective_id=0, has_side_effects=True, vmem_limit_bytes=60 * 2**20),
    )(tokens, expert_ids.T, gate_probs.T, w_gate, w_up, w_down)


def solution(mesh):
    in_specs = (
        P(("grp", "ep"), None),
        P(("grp", "ep"), None),
        P(("grp", "ep"), None),
        P(("ep", "hid"), None, None),
        P(("ep", "hid"), None, None),
        P(("ep", "hid"), None, None),
    )
    out_specs = P(("grp", "ep"), "hid")
    body = functools.partial(local, mesh.shape["ep"], mesh.shape["hid"])
    return jax.shard_map(body, mesh=mesh, in_specs=in_specs, out_specs=out_specs, check_vma=False)
```

```python
import functools

import jax
import jax.numpy as jnp
from jax import lax
from jax.experimental import pallas as pl
from jax.experimental.pallas import tpu as pltpu
from jax.sharding import PartitionSpec as P

QUARTERS = 4
IN_CHUNKS = 4
HAND_OVER = 1
HELD_BACK = 2
EARLY = (10, 2)
RETURN_STEP = 256
MESH = pl.DeviceIdType.MESH
F32 = jnp.float32
BF16 = jnp.bfloat16


def aligned(index, size):
    return pl.ds(pl.multiple_of(index * size, size), size)


def kernel(ep_count, hid_count, tokens_hbm, ids_hbm, probs_hbm, w_gate, w_up, w_down, out,
           tokens, ids, probs, gate_buf, up_buf, down_buf, key_t, combine, outgoing, sibling_out, slots,
           gate_acc, up_acc, hidden, partial, returned, mate_out, mate_in, far_out, far_in,
           load_sem, sib_sem, disp_send, disp_recv, fwd_send, fwd_recv, ret_send, ret_sib, ret_recv,
           mate_send, mate_recv, far_send, far_recv, here):
    ep = lax.axis_index("ep")
    hid = lax.axis_index("hid")
    groups = hid_count // QUARTERS
    group = hid // QUARTERS
    rows, width = tokens.shape
    picks = ids.shape[0]
    cap = slots.shape[1]
    half = width // 2
    pairs = ep_count // 2
    pair = ep // 2
    core = ep % 2
    sibling = pair * 2 + 1 - core
    side = hid % 2
    mate = hid + 1 - 2 * side
    columns = hid_count // 2
    column = hid // 2
    feat = width // hid_count
    chunks, step = returned.shape[1], returned.shape[4]
    wide = half // IN_CHUNKS

    barrier = pltpu.get_barrier_semaphore()
    for off in range(1, ep_count):
        pl.semaphore_signal(barrier, 1, device_id={"ep": lax.rem(ep + off, ep_count)}, device_id_type=MESH)
    pl.semaphore_signal(barrier, 1, device_id={"hid": mate}, device_id_type=MESH)
    relay = columns == 2
    across = jnp.clip(hid - 1 + 2 * side, 0, hid_count - 1)
    inner = (hid > 0) & (hid < hid_count - 1)
    if relay:
        @pl.when(inner)
        def _():
            pl.semaphore_signal(barrier, 1, device_id={"hid": across}, device_id_type=MESH)
    else:
        for off in range(1, columns):
            pl.semaphore_signal(barrier, 1, device_id={"hid": lax.rem(hid + 2 * off, hid_count)}, device_id_type=MESH)

    loads = [pltpu.make_async_copy(src, dst, load_sem.at[i])
             for i, (src, dst) in enumerate(((ids_hbm, ids), (probs_hbm, probs), (tokens_hbm, tokens),
                                             (w_gate.at[0], gate_buf), (w_up.at[0], up_buf), (w_down.at[0], down_buf)))]
    for load in loads[:3]:
        load.start()
    loads[0].wait()
    loads[1].wait()

    name = lax.broadcasted_iota(jnp.int32, (128, rows), 0) * groups + group
    count = jnp.zeros((128, rows), F32)
    weight = jnp.zeros((128, rows), F32)
    gate_round = probs[...].astype(BF16).astype(F32)
    for k in range(picks):
        hit = ids[k:k + 1, :] == name
        count = jnp.where(hit, 1.0, count)
        weight = jnp.where(hit, gate_round[k:k + 1, :], weight)
    earlier = (lax.broadcasted_iota(jnp.int32, (rows, rows), 0)
               < lax.broadcasted_iota(jnp.int32, (rows, rows), 1)).astype(F32).astype(BF16)
    before = jnp.dot(count.astype(BF16), earlier, preferred_element_type=F32)
    place = jnp.where(count > 0.5, before, -1000.0)
    key_t[...] = place.astype(jnp.int32)

    def pick_rows(first, blocks):
        row = lax.broadcasted_iota(jnp.int32, (cap, rows), 0)
        parts = [(key_t[pl.ds(first + b, 1), :] == row).astype(F32).astype(BF16) for b in range(blocks)]
        return jnp.concatenate(parts, axis=0) if blocks > 1 else parts[0]

    loads[2].wait()
    for load in loads[3:]:
        load.start()
    others = [lax.rem(pair + off, pairs) for off in range(1, pairs)]
    dispatch = [pltpu.make_async_remote_copy(
        src_ref=outgoing.at[i, to, :, pl.ds(k * wide, wide)],
        dst_ref=slots.at[ep, :, aligned(side * IN_CHUNKS + k, wide)],
        send_sem=disp_send.at[to, i, k], recv_sem=disp_recv.at[ep, k],
        device_id={"ep": 2 * other + to}, device_id_type=MESH)
        for k in range(IN_CHUNKS) for i, other in enumerate(others) for to in range(2)]
    chosen = [pick_rows(2 * other, 2) for other in others]
    for k in range(IN_CHUNKS):
        for i in range(pairs - 1):
            rows_out = jnp.dot(chosen[i], tokens[:, aligned(side * IN_CHUNKS + k, wide)], preferred_element_type=F32)
            outgoing[i, :, :, k * wide:(k + 1) * wide] = rows_out.astype(BF16).reshape(2, cap, wide)
        if k == 0:
            pl.semaphore_wait(barrier, ep_count + (inner.astype(jnp.int32) if relay else columns - 1))

        @pl.when(core == 0)
        def _():
            for copy in dispatch[2 * (pairs - 1) * k:2 * (pairs - 1) * (k + 1)]:
                copy.start()

    if relay:
        @pl.when(inner)
        def _():
            pl.semaphore_signal(here, 1, device_id={"hid": across}, device_id_type=MESH)
            pl.semaphore_signal(here, 1, device_id={"hid": mate}, device_id_type=MESH)

    sends = list(dispatch)
    tile = min(half, 512)
    chosen = pick_rows(sibling, 1)
    for col in range(0, width, tile):
        sibling_out[:, col:col + tile] = jnp.dot(
            chosen, tokens[:, col:col + tile], preferred_element_type=F32).astype(BF16)
    to_sibling = pltpu.make_async_remote_copy(
        src_ref=sibling_out, dst_ref=slots.at[ep], send_sem=sib_sem.at[0], recv_sem=sib_sem.at[1],
        device_id={"ep": sibling}, device_id_type=MESH)
    to_sibling.start()
    sends.append(to_sibling)
    chosen = pick_rows(ep, 1)
    for col in range(0, width, tile):
        slots[ep, :, col:col + tile] = jnp.dot(
            chosen, tokens[:, col:col + tile], preferred_element_type=F32).astype(BF16)

    lanes = lax.broadcasted_iota(jnp.int32, (rows, cap), 1)
    key = place.T.astype(jnp.int32)
    weight = weight.T
    for b in range(ep_count):
        combine[:, b * cap:(b + 1) * cap] = jnp.where(
            key[:, b:b + 1] == lanes, weight[:, b:b + 1], 0.0).astype(BF16)

    def activation(gate_act, up_act):
        return (gate_act / (1.0 + jnp.exp(-gate_act)) * up_act).astype(BF16)

    def act_step(stage, i, k, first=False, last=False):
        block = slots[2 * others[i] + stage, :, aligned(k, wide)]
        gate_act = jnp.dot(block, gate_buf[aligned(k, wide), :], preferred_element_type=F32)
        up_act = jnp.dot(block, up_buf[aligned(k, wide), :], preferred_element_type=F32)
        if not first:
            gate_act = gate_act + gate_acc[stage, i]
            up_act = up_act + up_acc[stage, i]
        if last:
            hidden[stage, others[i]] = activation(gate_act, up_act)
        else:
            gate_acc[stage, i] = gate_act
            up_acc[stage, i] = up_act

    pltpu.make_async_remote_copy(
        src_ref=sibling_out, dst_ref=slots.at[sibling], send_sem=sib_sem.at[0], recv_sem=sib_sem.at[1],
        device_id={"ep": sibling}, device_id_type=MESH).wait_recv()
    loads[3].wait()
    loads[4].wait()
    block = slots[pl.ds(2 * pair, 2)].reshape(2 * cap, width)
    value = activation(jnp.dot(block, gate_buf[...], preferred_element_type=F32),
                       jnp.dot(block, up_buf[...], preferred_element_type=F32))
    for stage in range(2):
        hidden[stage, pair] = value[stage * cap:(stage + 1) * cap]

    def forward(stage, i, k):
        landed = slots.at[2 * others[i] + stage, :, aligned(side * IN_CHUNKS + k, wide)]
        return pltpu.make_async_remote_copy(
            src_ref=landed, dst_ref=landed,
            send_sem=fwd_send.at[i, k, stage], recv_sem=fwd_recv.at[i, k, stage],
            device_id={"hid": mate}, device_id_type=MESH)

    def direct(stage, i, k):
        source = 2 * others[i] + stage
        landed = slots.at[source, :, aligned(side * IN_CHUNKS + k, wide)]
        pltpu.make_async_remote_copy(
            src_ref=landed, dst_ref=landed,
            send_sem=disp_send.at[0, i, k], recv_sem=disp_recv.at[source, k],
            device_id={"ep": source}, device_id_type=MESH).wait_recv()
        copy = forward(stage, i, k)
        copy.start()
        sends.append(copy)
        act_step(stage, i, side * IN_CHUNKS + k, first=k == 0)

    def relayed(stage, i, k):
        forward(stage, i, k).wait_recv()
        act_step(stage, i, (1 - side) * IN_CHUNKS + k, last=k == IN_CHUNKS - 1)

    pieces = [(i, k) for i in range(pairs - 1) for k in range(IN_CHUNKS)]

    elsewhere = [lax.rem(column + off, columns) for off in range(1, columns)]
    targets = [2 * c + 1 - side for c in elsewhere] + [2 * c + side for c in elsewhere] + [mate, hid]

    away = [(s, c) for s in range(columns - 1) for c in range(chunks)]
    for c in range(chunks):
        away += [(s, c) for s in range(columns - 1, 2 * columns - 1)]
    own = [(hid_count - 1, c) for c in range(chunks)]

    def give_back(stage, order):
        for s, c in order:
            target = targets[s]
            value = jnp.dot(hidden[stage].reshape(pairs * cap, -1), down_buf[:, aligned(target * chunks + c, step)],
                            preferred_element_type=F32)
            partial[stage, s, c] = value.astype(BF16).reshape(pairs, cap, step)
            for i, other in enumerate(others):
                copy = pltpu.make_async_remote_copy(
                    src_ref=partial.at[stage, s, c, other], dst_ref=returned.at[s, c, ep],
                    send_sem=ret_send.at[stage, s, c, i], recv_sem=ret_recv.at[s, c, ep],
                    device_id={"ep": 2 * other + stage}, device_id_type=MESH)
                copy.start()
                sends.append(copy)

        @pl.when(core == stage)
        def _():
            for s, c in order:
                returned[s, c, ep] = partial[stage, s, c, pair]

        @pl.when(core != stage)
        def _():
            for s, c in order:
                back_to_sibling(stage, s, c).start()

    def back_to_sibling(stage, s, c):
        return pltpu.make_async_remote_copy(
            src_ref=partial.at[stage, s, c, pair], dst_ref=returned.at[s, c, ep],
            send_sem=ret_sib.at[s, c], recv_sem=ret_recv.at[s, c, ep],
            device_id={"ep": sibling}, device_id_type=MESH)

    def to_mate(slot, c):
        return pltpu.make_async_remote_copy(
            src_ref=mate_out.at[slot, c], dst_ref=mate_in.at[slot, c],
            send_sem=mate_send.at[slot, c], recv_sem=mate_recv.at[slot, c],
            device_id={"hid": mate}, device_id_type=MESH)

    def to_far(slot, c, target):
        return pltpu.make_async_remote_copy(
            src_ref=far_out.at[slot, c], dst_ref=far_in.at[slot, c],
            send_sem=far_send.at[slot, c], recv_sem=far_recv.at[slot, c],
            device_id={"hid": target}, device_id_type=MESH)

    def gather(s, c):
        for off in range(1, ep_count):
            source = lax.rem(ep + off, ep_count)
            pltpu.make_async_remote_copy(
                src_ref=returned.at[s, c, source], dst_ref=returned.at[s, c, source],
                send_sem=ret_sib.at[s, c], recv_sem=ret_recv.at[s, c, source],
                device_id={"ep": source}, device_id_type=MESH).wait_recv()
        total = jnp.dot(combine[...], returned[s, c].reshape(ep_count * cap, step), preferred_element_type=F32)
        if s < columns - 1 or s == 2 * columns - 2:
            slot = s if s < columns - 1 else columns - 1
            mate_out[slot, c] = total.astype(BF16)
            copy = to_mate(slot, c)
        elif s < 2 * columns - 2:
            slot = s - (columns - 1)
            to_mate(slot, c).wait_recv()
            far_out[slot, c] = (total + mate_in[slot, c].astype(F32)).astype(BF16)
            copy = to_far(slot, c, targets[s])
        else:
            to_mate(columns - 1, c).wait_recv()
            total = total + mate_in[columns - 1, c].astype(F32)
            for slot in range(columns - 1):
                to_far(slot, c, targets[s]).wait_recv()
                total = total + far_in[slot, c].astype(F32)
            out[:, c * step:(c + 1) * step] = total.astype(BF16)
            return
        copy.start()
    def gather_on(which, order):
        @pl.when(core == which)
        def _():
            for s, c in order:
                gather(s, c)

    for n, piece in enumerate(pieces):
        direct(0, *piece)
        if n == HAND_OVER:
            @pl.when(core == 1)
            def _():
                for copy in dispatch:
                    copy.start()
    held = len(pieces) - HELD_BACK
    for n, piece in enumerate(pieces):
        relayed(0, *piece)
        if n < held:
            direct(1, *pieces[n])
    loads[5].wait()
    if relay:
        pl.semaphore_wait(here, 1)
    give_back(0, away)
    for piece in pieces[held:]:
        direct(1, *piece)
    first = EARLY[0]
    gather_on(0, away[:first])
    for piece in pieces:
        relayed(1, *piece)
    early = first + EARLY[1]
    gather_on(0, away[first:early])
    give_back(1, away)
    give_back(0, own)
    give_back(1, own)
    gather_on(1, away[:early])
    for s, c in away[early:] + own:
        gather(s, c)

    for s in range(hid_count):
        for c in range(chunks):
            back_to_sibling(1 - core, s, c).wait_send()
    for c in range(chunks):
        for slot in range(columns):
            to_mate(slot, c).wait_send()
        for slot in range(columns - 1):
            to_far(slot, c, targets[columns - 1 + slot]).wait_send()
    for copy in sends:
        copy.wait_send()


def local(ep_count, hid_count, tokens, expert_ids, gate_probs, w_gate, w_up, w_down):
    rows, width = tokens.shape
    inner = w_gate.shape[2]
    picks = expert_ids.shape[1]
    cap = rows // 2
    feat = width // hid_count
    step = min(RETURN_STEP, feat)
    chunks = feat // step
    pairs = ep_count // 2
    columns = hid_count // 2
    others = max(pairs - 1, 1)
    far = max(columns - 1, 1)
    hbm = pl.BlockSpec(memory_space=pl.ANY)
    dma = pltpu.SemaphoreType.DMA
    return pl.pallas_call(
        functools.partial(kernel, ep_count, hid_count),
        out_shape=pltpu.VMEM((rows, feat), BF16),
        in_specs=[hbm] * 6,
        out_specs=pl.BlockSpec(memory_space=pltpu.VMEM),
        scratch_shapes=[
            pltpu.VMEM((rows, width), BF16),
            pltpu.VMEM((picks, rows), jnp.int32),
            pltpu.VMEM((picks, rows), F32),
            pltpu.VMEM((width, inner), BF16),
            pltpu.VMEM((width, inner), BF16),
            pltpu.VMEM((inner, width), BF16),
            pltpu.VMEM((128, rows), jnp.int32),
            pltpu.VMEM((rows, ep_count * cap), BF16),
            pltpu.VMEM((others, 2, cap, width // 2), BF16),
            pltpu.VMEM((cap, width), BF16),
            pltpu.VMEM((ep_count, cap, width), BF16),
            pltpu.VMEM((2, others, cap, inner), F32),
            pltpu.VMEM((2, others, cap, inner), F32),
            pltpu.VMEM((2, pairs, cap, inner), BF16),
            pltpu.VMEM((2, hid_count, chunks, pairs, cap, step), BF16),
            pltpu.VMEM((hid_count, chunks, ep_count, cap, step), BF16),
            pltpu.VMEM((columns, chunks, rows, step), BF16),
            pltpu.VMEM((columns, chunks, rows, step), BF16),
            pltpu.VMEM((far, chunks, rows, step), BF16),
            pltpu.VMEM((far, chunks, rows, step), BF16),
            dma((6,)),
            dma((2,)),
            dma((2, others, IN_CHUNKS)),
            dma((ep_count, IN_CHUNKS)),
            dma((others, IN_CHUNKS, 2)),
            dma((others, IN_CHUNKS, 2)),
            dma((2, hid_count, chunks, others)),
            dma((hid_count, chunks)),
            dma((hid_count, chunks, ep_count)),
            dma((columns, chunks)),
            dma((columns, chunks)),
            dma((far, chunks)),
            dma((far, chunks)),
            pltpu.SemaphoreType.REGULAR,
        ],
        compiler_params=pltpu.CompilerParams(
            collective_id=0, has_side_effects=True, vmem_limit_bytes=60 * 2**20),
    )(tokens, expert_ids.T, gate_probs.T, w_gate, w_up, w_down)


def solution(mesh):
    in_specs = (
        P(("grp", "ep"), None),
        P(("grp", "ep"), None),
        P(("grp", "ep"), None),
        P(("ep", "hid"), None, None),
        P(("ep", "hid"), None, None),
        P(("ep", "hid"), None, None),
    )
    out_specs = P(("grp", "ep"), "hid")
    body = functools.partial(local, mesh.shape["ep"], mesh.shape["hid"])
    return jax.shard_map(body, mesh=mesh, in_specs=in_specs, out_specs=out_specs, check_vma=False)
```
